32 devices in a mesh: seq: 16 (over z, x, core), ch: 2 (over y).
Axes of the slice: x: 2, y: 2, z: 4, core: 2. Of those that a mesh axis runs over, the one named last changes fastest.
Arguments:
- out_grad: bfloat16 [2048, 4096], P('seq', 'ch'), may hold values from -6 to 6
- out_weight: bfloat16 [4096, 4096], P(('seq', 'ch')), may hold values from -0.09375 to 0.09375
- outer_gate: bfloat16 [2048, 4096], P('seq', 'ch'), may hold values from -6 to 6
- long_out: bfloat16 [2048, 4096], P('seq', 'ch'), may hold values from -6 to 6
- inner_gate: bfloat16 [2048, 4096], P('seq', 'ch'), may hold values from -6 to 6
- conv_input: bfloat16 [2048, 4096], P('seq', 'ch'), may hold values from -6 to 6
- short_out: bfloat16 [2048, 4096], P('seq', 'ch'), may hold values from -6 to 6
- medium_out: bfloat16 [2048, 4096], P('seq', 'ch'), may hold values from -6 to 6
- long_filter: bfloat16 [2048, 4096], P('seq', 'ch'), may hold values from -6 to 6
- taps_short: bfloat16 [7, 4096], P(None, 'ch'), may hold values from -2 to 2
- taps_medium: bfloat16 [128, 4096], P(None, 'ch'), may hold values from -0.5 to 0.5
Outputs:
- grad_outer: bfloat16 [2048, 4096], P('seq', 'ch')
- grad_inner: bfloat16 [2048, 4096], P('seq', 'ch')
- grad_input: bfloat16 [2048, 4096], P('seq', 'ch')
- grad_filter: float32 [2048, 4096], P('seq', 'ch')
- grad_short: float32 [7, 4096], P(None, 'ch')
- grad_medium: float32 [128, 4096], P(None, 'ch')
The draws below stay inside these ranges and needn't reach their ends.
All inputs are finite; a program needn't handle non-finite values.
Results may differ from the reference program's by a relative error of at most 0.0065.
Values may be sent and summed in bfloat16 or wider, within the bound.
No kernel may reach another device: no remote copies, remote signals or barrier semaphores. Data moves between devices by JAX's collectives and lax.ppermute only.
A program may use at most 128 MiB of HBM per device.

```python
import jax
import jax.numpy as jnp

D = 4096
SHORT = 7
MEDIUM = 128
NTOK = 2048


def level_of(key, extent, cuts, smallest, high):
    def one(position, shards_of):
        heights = jax.random.uniform(jax.random.fold_in(jax.random.fold_in(key, 6), position), (shards_of,), jnp.float32, smallest / len(cuts), high / len(cuts))
        return jnp.repeat(jnp.exp(heights), extent[position] // shards_of).reshape((-1,) + (1,) * (len(extent) - position - 1))

    gain = one(*cuts[0])
    for cut in cuts[1:]:
        gain = gain * one(*cut)
    return gain


def noise(rng, extent, spread, bound, shards=(), held_as=jnp.bfloat16):
    drawn = spread * jax.random.normal(rng, extent, jnp.float32)
    if shards:
        drawn = drawn * level_of(rng, extent, shards, -0.22, 0.18)
    return jnp.clip(drawn, -bound, bound).astype(held_as)


def setup_inputs(seed: int = 0) -> dict:
    key_list = jax.random.split(jax.random.key(seed), 12)
    return {
        "out_grad": noise(key_list[0], (NTOK, D), 1.0, 6.0, ((0, 16), (1, 2))),
        "out_weight": noise(key_list[1], (D, D), D ** -0.5, 0.09375, ((0, 32),)),
        "outer_gate": noise(key_list[2], (NTOK, D), 1.0, 6.0, ((0, 16), (1, 2))),
        "long_out": noise(key_list[3], (NTOK, D), 1.0, 6.0, ((0, 16), (1, 2))),
        "inner_gate": noise(key_list[4], (NTOK, D), 1.0, 6.0, ((0, 16), (1, 2))),
        "conv_input": noise(key_list[5], (NTOK, D), 1.0, 6.0, ((0, 16), (1, 2))),
        "short_out": noise(key_list[6], (NTOK, D), 1.0, 6.0, ((0, 16), (1, 2))),
        "medium_out": noise(key_list[7], (NTOK, D), 1.0, 6.0, ((0, 16), (1, 2))),
        "long_filter": noise(key_list[8], (NTOK, D), 1.0, 6.0, ((0, 16), (1, 2))),
        "taps_short": noise(key_list[9], (SHORT, D), SHORT ** -0.5, 2.0, ((1, 2),)),
        "taps_medium": noise(key_list[10], (MEDIUM, D), MEDIUM ** -0.5, 0.5, ((1, 2),)),
    }


def correlate(first, second):
    length = second.shape[0]
    first_spec = jnp.fft.rfft(first.astype(jnp.float32), n=2 * length, axis=0)
    second_spec = jnp.fft.rfft(second.astype(jnp.float32), n=2 * length, axis=0)
    return jnp.fft.irfft(jnp.conj(first_spec) * second_spec, n=2 * length, axis=0)[:length]


def adjoint_taps(grads, taps):
    return correlate(taps, grads)


def tap_products(grads, values, count):
    return correlate(values, grads)[:count]


def reference(out_grad, out_weight, outer_gate, long_out, inner_gate, conv_input, short_out, medium_out, long_filter, taps_short, taps_medium):
    factor = NTOK ** -0.5
    hidden = jnp.dot(out_grad, out_weight, preferred_element_type=jnp.float32)
    grad_outer = (hidden * long_out.astype(jnp.float32)).astype(jnp.bfloat16)
    long_grad = (hidden * outer_gate.astype(jnp.float32)).astype(jnp.bfloat16)
    product = (inner_gate.astype(jnp.float32) * medium_out.astype(jnp.float32)).astype(jnp.bfloat16)
    point_grad = factor * correlate(long_filter, long_grad)
    grad_filter = factor * correlate(product, long_grad)
    medium_grad = (point_grad * inner_gate.astype(jnp.float32)).astype(jnp.bfloat16)
    grad_inner = (point_grad * medium_out.astype(jnp.float32)).astype(jnp.bfloat16)
    short_grad = adjoint_taps(medium_grad, taps_medium).astype(jnp.bfloat16)
    grad_input = adjoint_taps(short_grad, taps_short).astype(jnp.bfloat16)
    grad_medium = factor * tap_products(medium_grad, short_out, MEDIUM)
    grad_short = factor * tap_products(short_grad, conv_input, SHORT)
    return grad_outer, grad_inner, grad_input, grad_filter, grad_short, grad_medium
```

```python
import functools
import math

import jax
import jax.numpy as jnp
from jax import lax
from jax.experimental import pallas as pl
from jax.experimental.pallas import tpu as pltpu
from jax.sharding import Mesh, PartitionSpec as P


BLOCK = 256
UNROLL = 8
LANES = 128
SUB = 8
BF16 = jnp.bfloat16
F32 = jnp.float32
VMEM_LIMIT = 60 * 1024 * 1024


def table(block):
    row = lax.iota(jnp.int32, 2 * block)[:, None]
    slot = row % block
    freq = jnp.where(slot < block // 2, 2 * slot, 2 * (slot - block // 2) + 1)
    time = lax.iota(jnp.int32, block)[None, :]
    angle = (((2 * freq + 1) * time) % (4 * block)).astype(F32) * (math.pi / (2 * block))
    full = jnp.where(row < block, jnp.cos(angle), -jnp.sin(angle))
    high = lax.reduce_precision(full, 8, 7)
    low = full - high
    return high.astype(BF16), low.astype(BF16)


def dot(left, right):
    return jnp.dot(left, right, preferred_element_type=F32)


def forward(ftab_ref, value):
    both = dot(ftab_ref[...], value)
    half = both.shape[0] // 2
    return both[:half] + both[half:]


def inverse(itab_ref, spectrum, count):
    high = spectrum.astype(BF16)
    low = (spectrum - high.astype(F32)).astype(BF16)
    both = dot(itab_ref[...], high)
    return both[:count] + both[count:] + dot(itab_ref[:count], low)


def each(count, body):
    if count <= UNROLL:
        for index in range(count):
            body(index)
    else:

        def step(index, carry):
            body(index)
            return carry

        lax.fori_loop(0, count, step, 0)


def join(spec_ref):
    blocks, double, _ = spec_ref.shape
    block = double // 2

    def chunk(r, carry):
        rows = pl.ds(pl.multiple_of(r * SUB, SUB), SUB)
        irows = pl.ds(pl.multiple_of(block + r * SUB, SUB), SUB)
        sign = jnp.where(r < block // (2 * SUB), 1.0, -1.0).astype(F32)

        def step(s):
            real = spec_ref[s + 1, rows, :]
            imag = spec_ref[s + 1, irows, :]
            spec_ref[s, rows, :] = spec_ref[s, rows, :] + sign * imag
            spec_ref[s, irows, :] = spec_ref[s, irows, :] - sign * real

        each(blocks - 1, step)
        return carry

    lax.fori_loop(0, block // SUB, chunk, 0)


def conj_times(left, right):
    return left[0] * right[0] + left[1] * right[1], left[0] * right[1] - left[1] * right[0]


def correlate(spec_ref, joined_ref, hold_ref):
    blocks, double, lanes = spec_ref.shape
    block = double // 2

    def chunk(r, carry):
        rows = pl.ds(pl.multiple_of(r * SUB, SUB), SUB)
        irows = pl.ds(pl.multiple_of(block + r * SUB, SUB), SUB)

        def pair(ref, s):
            return ref[s, rows, :], ref[s, irows, :]

        if blocks <= UNROLL:
            left = [pair(spec_ref, c) for c in range(blocks)]
            right = [pair(joined_ref, c) for c in range(blocks)]
            for a in range(blocks):
                real, imag = conj_times(left[0], right[a])
                for c in range(1, blocks - a):
                    more = conj_times(left[c], right[a + c])
                    real, imag = real + more[0], imag + more[1]
                spec_ref[a, rows, :] = real
                spec_ref[a, irows, :] = imag
        else:

            def keep(c):
                hold_ref[c, :SUB, :], hold_ref[c, SUB:, :] = pair(spec_ref, c)

            def row(a):
                def term(c, sums):
                    left = hold_ref[c, :SUB, :], hold_ref[c, SUB:, :]
                    more = conj_times(left, pair(joined_ref, a + c))
                    return sums[0] + more[0], sums[1] + more[1]

                zero = jnp.zeros((SUB, lanes), F32)
                real, imag = lax.fori_loop(0, blocks - a, term, (zero, zero))
                spec_ref[a, rows, :] = real
                spec_ref[a, irows, :] = imag

            each(blocks, keep)
            each(blocks, row)
        return carry

    lax.fori_loop(0, block // SUB, chunk, 0)


def block_rows(ref, s, block):
    start = s * block
    if not isinstance(start, int):
        start = pl.multiple_of(start, block)
    return ref[pl.ds(start, block), :]


def set_rows(ref, s, block, value):
    start = s * block
    if not isinstance(start, int):
        start = pl.multiple_of(start, block)
    ref[pl.ds(start, block), :] = value


def long_kernel(scale, saved_ref, grad_ref, ftab_ref, itab_ref, medium_ref, out_ref, filt, prod, grad, hold):
    blocks, double, lanes = filt.shape
    block = double // 2
    height = saved_ref.shape[2]
    many = block // height

    def part(index, s):
        return saved_ref[pl.ds(s * many, many), index].reshape(block, lanes)

    def spread(s):
        product = (part(1, s).astype(F32) * part(2, s).astype(F32)).astype(BF16)
        spectrum = forward(ftab_ref, jnp.concatenate([part(0, s), product], axis=1))
        filt[s] = spectrum[:, :lanes]
        prod[s] = spectrum[:, lanes:]

    def spread_grad(s):
        value = [block_rows(grad_ref, 2 * s + half, block) for half in range(2)]
        spectrum = forward(ftab_ref, jnp.concatenate(value, axis=1))
        grad[2 * s] = spectrum[:, :lanes]
        grad[2 * s + 1] = spectrum[:, lanes:]

    def finish(a):
        time = inverse(itab_ref, jnp.concatenate([filt[a], prod[a]], axis=1), block) * scale
        point = time[:, :lanes]
        set_rows(medium_ref, a, block, (point * part(1, a).astype(F32)).astype(BF16))
        inner = (point * part(2, a).astype(F32)).astype(BF16)
        out_ref[pl.ds(a * many, many), 0] = inner.reshape(many, height, lanes)
        outer = time[:, lanes:].astype(BF16)
        out_ref[pl.ds(a * many, many), 1] = outer.reshape(many, height, lanes)

    each(blocks, spread)
    each(blocks // 2, spread_grad)
    join(grad)
    correlate(filt, grad, hold)
    correlate(prod, grad, hold)
    each(blocks, finish)


def short_kernel(
    scale,
    factor,
    grad_ref,
    saved_ref,
    medium_ref,
    short_ref,
    ftab_ref,
    itab_ref,
    out_ref,
    taps_ref,
    grad,
    saved,
    taps,
    tail,
):
    blocks, double, lanes = grad.shape
    block = double // 2
    height = saved_ref.shape[2]
    many = block // height
    medium = medium_ref.shape[0]
    short = short_ref.shape[0]
    total = blocks * block

    def spread(s):
        part = saved_ref[pl.ds(s * many, many), 3].reshape(block, lanes)
        value = jnp.concatenate([block_rows(grad_ref, s, block), part], axis=1)
        spectrum = forward(ftab_ref, value)
        grad[s] = spectrum[:, :lanes]
        saved[s] = spectrum[:, lanes:]

    each(blocks, spread)
    padded = jnp.concatenate([medium_ref[...], jnp.zeros((block - medium, lanes), BF16)], axis=0)
    taps[...] = forward(ftab_ref, padded)
    join(grad)

    def chunk(r, carry):
        rows = pl.ds(pl.multiple_of(r * SUB, SUB), SUB)
        irows = pl.ds(pl.multiple_of(block + r * SUB, SUB), SUB)
        tap = taps[rows, :], taps[irows, :]

        def term(s, sums):
            right = grad[s, rows, :], grad[s, irows, :]
            more = conj_times((saved[s, rows, :], saved[s, irows, :]), right)
            grad[s, rows, :], grad[s, irows, :] = conj_times(tap, right)
            return sums[0] + more[0], sums[1] + more[1]

        zero = jnp.zeros((SUB, lanes), F32)
        sums = (zero, zero)
        if blocks <= UNROLL:
            for s in range(blocks):
                sums = term(s, sums)
        else:
            sums = lax.fori_loop(0, blocks, term, sums)
        taps[rows, :], taps[irows, :] = sums
        return carry

    lax.fori_loop(0, block // SUB, chunk, 0)
    tap_grad = inverse(itab_ref, taps[...], block)[:medium] * (scale * factor)

    def finish(s):
        pair = jnp.concatenate([grad[2 * s], grad[2 * s + 1]], axis=1)
        time = inverse(itab_ref, pair, block) * scale
        for half in range(2):
            value = time[:, half * lanes : (half + 1) * lanes].astype(BF16).astype(F32)
            set_rows(tail, 2 * s + half, block, value)

    each(blocks // 2, finish)
    tail[total : total + 2 * SUB, :] = jnp.zeros((2 * SUB, lanes), F32)

    def span(b, sums):
        base = pl.multiple_of(b * height, height)
        values = saved_ref[b, 4].astype(F32)
        result = jnp.zeros((height, lanes), F32)
        new = []
        for j in range(short):
            shifted = tail[pl.ds(base + j, height), :]
            result = result + short_ref[j : j + 1, :].astype(F32) * shifted
            pieces = (values * shifted).reshape(height // SUB, SUB, lanes)
            new.append(sums[j] + jnp.sum(pieces, axis=0))
        out_ref[b] = result.astype(BF16)
        return tuple(new)

    start = tuple(jnp.zeros((SUB, lanes), F32) for _ in range(short))
    sums = lax.fori_loop(0, total // height, span, start)
    rows = [jnp.sum(value, axis=0, keepdims=True) * factor for value in sums]
    rest = taps_ref.shape[0] - medium
    rows.append(jnp.zeros((rest - short, lanes), F32))
    taps_ref[:medium, :] = tap_grad.astype(BF16)
    taps_ref[medium:, :] = jnp.concatenate(rows, axis=0).astype(BF16)


def call(kernel, outs, scratch, flops, *args):
    vmem = pl.BlockSpec(memory_space=pltpu.VMEM)
    return pl.pallas_call(
        kernel,
        out_shape=outs,
        in_specs=[vmem] * len(args),
        out_specs=jax.tree.map(lambda _: vmem, outs),
        scratch_shapes=scratch,
        compiler_params=pltpu.CompilerParams(vmem_limit_bytes=VMEM_LIMIT),
        cost_estimate=pl.CostEstimate(flops=flops, bytes_accessed=1 << 23, transcendentals=0),
    )(*args)


def pack_kernel(*refs):
    *ins, out_ref = refs
    outer, _, _, _, narrow = out_ref.shape
    for index, ref in enumerate(ins):
        for o in range(outer):
            out_ref[o, 0, index] = ref[:, o * narrow : (o + 1) * narrow]


def pack(values, outer, inner):
    height, channels = values[0].shape
    narrow = channels // (outer * inner)
    wide = channels // inner
    shape = (outer, inner, len(values), height, narrow)
    return pl.pallas_call(
        pack_kernel,
        out_shape=jax.ShapeDtypeStruct(shape, values[0].dtype),
        grid=(inner,),
        in_specs=[pl.BlockSpec((height, wide), lambda i: (0, i))] * len(values),
        out_specs=pl.BlockSpec((outer, 1) + shape[2:], lambda i: (0, i, 0, 0, 0)),
        cost_estimate=pl.CostEstimate(flops=1 << 28, bytes_accessed=1 << 22, transcendentals=0),
    )(*values)


def unpack_kernel(places, in_ref, *out_refs):
    _, outer, _, narrow = in_ref.shape
    for (start, count), out_ref in zip(places, out_refs):
        for o in range(outer):
            part = in_ref[0, o, start : start + count].astype(out_ref.dtype)
            out_ref[:, o * narrow : (o + 1) * narrow] = part


def unpack(value, order, *outs):
    inner, outer, length, narrow = value.shape
    wide = outer * narrow
    return pl.pallas_call(
        functools.partial(unpack_kernel, tuple(out[:2] for out in outs)),
        out_shape=[jax.ShapeDtypeStruct((count, wide * inner), kind) for _, count, kind in outs],
        grid=(inner,),
        in_specs=[pl.BlockSpec((1, outer, length, narrow), lambda i: (order(i), 0, 0, 0))],
        out_specs=[pl.BlockSpec((count, wide), lambda i: (0, i)) for _, count, _ in outs],
        cost_estimate=pl.CostEstimate(flops=1 << 28, bytes_accessed=1 << 22, transcendentals=0),
    )(value)


def unpack_devices(value, outer, inner, *outs):
    _, length, narrow = value.shape
    wide = outer * narrow

    def kernel(in_ref, *out_refs):
        for (start, count, _), out_ref in zip(outs, out_refs):
            for o in range(outer):
                part = in_ref[o, 0, start : start + count].astype(out_ref.dtype)
                out_ref[:, o * narrow : (o + 1) * narrow] = part

    return pl.pallas_call(
        kernel,
        out_shape=[jax.ShapeDtypeStruct((count, wide * inner), kind) for _, count, kind in outs],
        grid=(inner,),
        in_specs=[pl.BlockSpec((outer, 1, length, narrow), lambda i: (0, i, 0, 0))],
        out_specs=[pl.BlockSpec((count, wide), lambda i: (0, i)) for _, count, _ in outs],
        cost_estimate=pl.CostEstimate(flops=1 << 28, bytes_accessed=1 << 22, transcendentals=0),
    )(value.reshape(outer, inner, length, narrow))


def gather(value, axis):
    count = lax.axis_size(axis)
    place = lax.axis_index(axis)
    result = jnp.stack([value] * count)
    for step in range(1, count):
        more = lax.ppermute(value, axis, [(s, (s + step) % count) for s in range(count)])
        result = lax.dynamic_update_index_in_dim(result, more, (place - step) % count, 0)
    return result


def trade(value, axis, dim):
    count = lax.axis_size(axis)
    place = lax.axis_index(axis)
    result = value
    for step in range(1, count):
        sent = lax.dynamic_index_in_dim(value, (place + step) % count, dim, keepdims=True)
        got = lax.ppermute(sent, axis, [(s, (s + step) % count) for s in range(count)])
        result = lax.dynamic_update_slice_in_dim(result, got, (place - step) % count, dim)
    return result


def swap(value, axes):
    return lax.all_to_all(value, axes, split_axis=0, concat_axis=0, tiled=True)


def per_device(
    out_grad,
    out_weight,
    outer_gate,
    long_out,
    inner_gate,
    conv_input,
    short_out,
    medium_out,
    long_filter,
    taps_short,
    taps_medium,
):
    height, channels = outer_gate.shape
    halves, lines, pairs, cores = (lax.axis_size(axis) for axis in ("h", "l", "j", "k"))
    groups = lax.axis_size("ch")
    outer = halves * lines
    inner = pairs * cores
    devices = outer * inner
    total = height * devices
    narrow = channels // devices
    wide = channels // inner
    medium, short = taps_medium.shape[0], taps_short.shape[0]
    planes = ("h", "l")
    seq = planes + ("j", "k")
    half, line = lax.axis_index("h"), lax.axis_index("l")
    me = half * lines + line
    my_inner = lax.axis_index("j") * cores + lax.axis_index("k")

    saved = pack([long_filter, inner_gate, medium_out, short_out, conv_input], outer, inner)
    saved = swap(saved.reshape((devices,) + saved.shape[2:]), seq)

    rows = out_weight.shape[0]
    depth = inner * groups * rows

    def to_columns(value):
        value = value.reshape(rows, groups, pairs, cores, wide).transpose(2, 3, 1, 0, 4)
        for axis, dim in (("j", 0), ("ch", 2), ("k", 1)):
            value = trade(value, axis, dim)
        return value.reshape(depth, wide)

    blocks = [(to_columns(out_weight), line)]
    for step in range(1, lines):
        shift = [(s, (s + step) % lines) for s in range(lines)]
        more = lax.ppermute(out_weight, "l", shift)
        blocks.append((to_columns(more), (line - step) % lines))

    both = gather(out_grad, "ch")
    share = height // groups
    first = lax.axis_index("ch") * share
    piece = lax.dynamic_slice(both, (1 - half, first, 0), (1, share, channels))
    piece = lax.ppermute(piece[0], "h", [(0, 1), (1, 0)])
    piece = gather(piece, "ch").reshape(height, channels)
    mine = lax.dynamic_index_in_dim(both, half, 0, keepdims=False)
    mine = gather(gather(mine, "j"), "k")
    mine = mine.reshape(inner * height, channels)
    other = gather(gather(piece, "j"), "k")
    other = other.reshape(inner * height, channels)

    def term(value, block, source):
        return dot(lax.dynamic_slice_in_dim(value, source * depth, depth, 1), block)

    away = sum(term(other, block, source) for block, source in blocks).astype(BF16)
    away = lax.ppermute(away, "h", [(0, 1), (1, 0)])
    hidden = sum(term(mine, block, source) for block, source in blocks) + away.astype(F32)
    hidden = hidden.reshape(cores, pairs, height, wide).transpose(1, 0, 2, 3)

    def to_plane(value):
        return value.reshape(height, pairs, cores, wide).transpose(1, 2, 0, 3)

    gates = jnp.stack([to_plane(outer_gate), to_plane(long_out)], axis=2)
    gates = trade(trade(gates, "j", 0), "k", 1).astype(F32)
    long_grad = (hidden * gates[:, :, 0]).astype(BF16).reshape(inner * height, outer, narrow)
    long_grad, saved = lax.optimization_barrier((long_grad.transpose(1, 0, 2), saved))
    long_grad = swap(long_grad, planes).reshape(total, narrow)
    grad_outer = (hidden * gates[:, :, 1]).astype(BF16)
    grad_outer = trade(trade(grad_outer, "j", 0), "k", 1)
    grad_outer = grad_outer.transpose(2, 0, 1, 3).reshape(height, channels)

    first = (my_inner * outer + me) * narrow
    my_medium = lax.dynamic_slice_in_dim(taps_medium, first, narrow, 1)
    my_short = lax.dynamic_slice_in_dim(taps_short, first, narrow, 1)

    saved = jnp.pad(saved, [(0, 0)] * 3 + [(0, -narrow % LANES)])
    lanes = -(-narrow // LANES) * LANES

    def pad(value):
        return jnp.pad(value, [(0, 0)] * (value.ndim - 1) + [(0, lanes - narrow)])

    block = max(height, min(BLOCK, total // 2))
    blocks = total // block
    high, low = table(block)
    ftab = jnp.concatenate([high, low])
    itab = jnp.concatenate([high.T, low.T])
    factor = total ** (-0.5)
    spectra = pltpu.VMEM((blocks, 2 * block, lanes), F32)
    hold = pltpu.VMEM((blocks, 2 * SUB, lanes), F32)
    out = jax.ShapeDtypeStruct
    medium_grad, sent_long = call(
        functools.partial(long_kernel, factor / block),
        (out((total, lanes), BF16), out((devices, 2, height, lanes), BF16)),
        [spectra] * 3 + [hold],
        24 * 2 * block * total * lanes,
        saved,
        pad(long_grad),
        ftab,
        itab,
    )
    rest = -(-short // 16) * 16
    sent_short, tap_grads = call(
        functools.partial(short_kernel, 1.0 / block, factor),
        (out((devices, height, lanes), BF16), out((medium + rest, lanes), BF16)),
        [spectra] * 2
        + [pltpu.VMEM((2 * block, lanes), F32), pltpu.VMEM((total + 2 * SUB, lanes), F32)],
        16 * 2 * block * total * lanes,
        medium_grad,
        saved,
        pad(my_medium),
        pad(my_short),
        ftab,
        itab,
    )
    sent_long = sent_long.reshape(devices, 2 * height, lanes)
    got_long = swap(sent_long[..., :narrow], seq)
    tap_grads = tap_grads[:, :narrow]
    for axis in ("l", "h", "j", "k"):
        tap_grads = gather(tap_grads, axis)
    got_long, sent_short = lax.optimization_barrier((got_long, sent_short))
    grad_inner, grad_filter = unpack_devices(
        got_long, outer, inner, (0, height, BF16), (height, height, F32)
    )
    got_short = swap(sent_short[..., :narrow], seq)
    (grad_input,) = unpack_devices(got_short, outer, inner, (0, height, BF16))
    grad_medium, grad_short = unpack(
        tap_grads.reshape(inner, outer, -1, narrow),
        lambda i: i % cores * pairs + i // cores,
        (0, medium, F32),
        (medium, short, F32),
    )
    return grad_outer, grad_inner, grad_input, grad_filter, grad_short, grad_medium


def solution(mesh):
    devices, groups = mesh.shape["seq"], mesh.shape["ch"]
    inner = 2 ** ((devices.bit_length() - 1) // 2)
    cores = min(2, inner)
    fine = Mesh(
        mesh.devices.reshape(2, devices // inner // 2, inner // cores, cores, groups),
        ("h", "l", "j", "k", "ch"),
    )
    seq = ("h", "l", "j", "k")
    tokens = P(seq, "ch")
    taps = P(None, "ch")

    return jax.shard_map(
        per_device,
        mesh=fine,
        in_specs=(tokens, P(seq + ("ch",), None)) + (tokens,) * 7 + (taps, taps),
        out_specs=(tokens,) * 4 + (taps, taps),
        check_vma=False,
    )
```

```python
import functools
import math

import jax
import jax.numpy as jnp
from jax import lax
from jax.experimental import pallas as pl
from jax.experimental.pallas import tpu as pltpu
from jax.sharding import Mesh, PartitionSpec as P


BLOCK = 256
UNROLL = 8
LANES = 128
SUB = 8
BF16 = jnp.bfloat16
F32 = jnp.float32
VMEM_LIMIT = 60 * 1024 * 1024


def table(block):
    row = lax.iota(jnp.int32, 2 * block)[:, None]
    slot = row % block
    freq = jnp.where(slot < block // 2, 2 * slot, 2 * (slot - block // 2) + 1)
    time = lax.iota(jnp.int32, block)[None, :]
    angle = (((2 * freq + 1) * time) % (4 * block)).astype(F32) * (math.pi / (2 * block))
    full = jnp.where(row < block, jnp.cos(angle), -jnp.sin(angle))
    high = lax.reduce_precision(full, 8, 7)
    low = full - high
    return high.astype(BF16), low.astype(BF16)


def dot(left, right):
    return jnp.dot(left, right, preferred_element_type=F32)


def forward(ftab_ref, value):
    both = dot(ftab_ref[...], value)
    half = both.shape[0] // 2
    return both[:half] + both[half:]


def inverse(itab_ref, spectrum, count):
    high = spectrum.astype(BF16)
    low = (spectrum - high.astype(F32)).astype(BF16)
    both = dot(itab_ref[...], high)
    return both[:count] + both[count:] + dot(itab_ref[:count], low)


def each(count, body):
    if count <= UNROLL:
        for index in range(count):
            body(index)
    else:

        def step(index, carry):
            body(index)
            return carry

        lax.fori_loop(0, count, step, 0)


def join(spec_ref):
    blocks, double, _ = spec_ref.shape
    block = double // 2

    def chunk(r, carry):
        rows = pl.ds(pl.multiple_of(r * SUB, SUB), SUB)
        irows = pl.ds(pl.multiple_of(block + r * SUB, SUB), SUB)
        sign = jnp.where(r < block // (2 * SUB), 1.0, -1.0).astype(F32)

        def step(s):
            real = spec_ref[s + 1, rows, :]
            imag = spec_ref[s + 1, irows, :]
            spec_ref[s, rows, :] = spec_ref[s, rows, :] + sign * imag
            spec_ref[s, irows, :] = spec_ref[s, irows, :] - sign * real

        each(blocks - 1, step)
        return carry

    lax.fori_loop(0, block // SUB, chunk, 0)


def conj_times(left, right):
    return left[0] * right[0] + left[1] * right[1], left[0] * right[1] - left[1] * right[0]


def correlate(spec_ref, joined_ref, hold_ref):
    blocks, double, lanes = spec_ref.shape
    block = double // 2

    def chunk(r, carry):
        rows = pl.ds(pl.multiple_of(r * SUB, SUB), SUB)
        irows = pl.ds(pl.multiple_of(block + r * SUB, SUB), SUB)

        def pair(ref, s):
            return ref[s, rows, :], ref[s, irows, :]

        if blocks <= UNROLL:
            left = [pair(spec_ref, c) for c in range(blocks)]
            right = [pair(joined_ref, c) for c in range(blocks)]
            for a in range(blocks):
                real, imag = conj_times(left[0], right[a])
                for c in range(1, blocks - a):
                    more = conj_times(left[c], right[a + c])
                    real, imag = real + more[0], imag + more[1]
                spec_ref[a, rows, :] = real
                spec_ref[a, irows, :] = imag
        else:

            def keep(c):
                hold_ref[c, :SUB, :], hold_ref[c, SUB:, :] = pair(spec_ref, c)

            def row(a):
                def term(c, sums):
                    left = hold_ref[c, :SUB, :], hold_ref[c, SUB:, :]
                    more = conj_times(left, pair(joined_ref, a + c))
                    return sums[0] + more[0], sums[1] + more[1]

                zero = jnp.zeros((SUB, lanes), F32)
                real, imag = lax.fori_loop(0, blocks - a, term, (zero, zero))
                spec_ref[a, rows, :] = real
                spec_ref[a, irows, :] = imag

            each(blocks, keep)
            each(blocks, row)
        return carry

    lax.fori_loop(0, block // SUB, chunk, 0)


def block_rows(ref, s, block):
    start = s * block
    if not isinstance(start, int):
        start = pl.multiple_of(start, block)
    return ref[pl.ds(start, block), :]


def set_rows(ref, s, block, value):
    start = s * block
    if not isinstance(start, int):
        start = pl.multiple_of(start, block)
    ref[pl.ds(start, block), :] = value


def part(ref, index, s, many):
    value = ref[pl.ds(s * many, many), index]
    return value.reshape(many * value.shape[1], value.shape[2])


def long_kernel(
    scale, gates_ref, filter_ref, grad_ref, ftab_ref, itab_ref, medium_ref, out_ref,
    filt, prod, grad, hold,
):
    blocks, double, lanes = filt.shape
    block = double // 2
    height = gates_ref.shape[2]
    many = block // height

    def spread(s):
        inner, medium = (part(gates_ref, index, s, many).astype(F32) for index in range(2))
        value = [part(filter_ref, 0, s, many), (inner * medium).astype(BF16)]
        spectrum = forward(ftab_ref, jnp.concatenate(value, axis=1))
        filt[s] = spectrum[:, :lanes]
        prod[s] = spectrum[:, lanes:]

    def spread_grad(s):
        value = [block_rows(grad_ref, 2 * s + side, block) for side in range(2)]
        spectrum = forward(ftab_ref, jnp.concatenate(value, axis=1))
        grad[2 * s] = spectrum[:, :lanes]
        grad[2 * s + 1] = spectrum[:, lanes:]

    def finish(a):
        time = inverse(itab_ref, jnp.concatenate([filt[a], prod[a]], axis=1), block) * scale
        point = time[:, :lanes]
        inner, medium = (part(gates_ref, index, a, many).astype(F32) for index in range(2))
        set_rows(medium_ref, a, block, (point * inner).astype(BF16))
        inner = (point * medium).astype(BF16)
        out_ref[pl.ds(a * many, many), 0] = inner.reshape(many, height, lanes)
        outer = time[:, lanes:].astype(BF16)
        out_ref[pl.ds(a * many, many), 1] = outer.reshape(many, height, lanes)

    each(blocks, spread)
    each(blocks // 2, spread_grad)
    join(grad)
    correlate(filt, grad, hold)
    correlate(prod, grad, hold)
    each(blocks, finish)


def short_kernel(
    scale,
    factor,
    grad_ref,
    saved_ref,
    medium_ref,
    short_ref,
    ftab_ref,
    itab_ref,
    out_ref,
    taps_ref,
    grad,
    saved,
    taps,
    tail,
):
    blocks, double, lanes = grad.shape
    block = double // 2
    height = saved_ref.shape[2]
    many = block // height
    medium = medium_ref.shape[0]
    short = short_ref.shape[0]
    total = blocks * block

    def spread(s):
        value = [block_rows(grad_ref, s, block), part(saved_ref, 0, s, many)]
        value = jnp.concatenate(value, axis=1)
        spectrum = forward(ftab_ref, value)
        grad[s] = spectrum[:, :lanes]
        saved[s] = spectrum[:, lanes:]

    each(blocks, spread)
    padded = jnp.concatenate([medium_ref[...], jnp.zeros((block - medium, lanes), BF16)], axis=0)
    taps[...] = forward(ftab_ref, padded)
    join(grad)

    def chunk(r, carry):
        rows = pl.ds(pl.multiple_of(r * SUB, SUB), SUB)
        irows = pl.ds(pl.multiple_of(block + r * SUB, SUB), SUB)
        tap = taps[rows, :], taps[irows, :]

        def term(s, sums):
            right = grad[s, rows, :], grad[s, irows, :]
            more = conj_times((saved[s, rows, :], saved[s, irows, :]), right)
            grad[s, rows, :], grad[s, irows, :] = conj_times(tap, right)
            return sums[0] + more[0], sums[1] + more[1]

        zero = jnp.zeros((SUB, lanes), F32)
        sums = (zero, zero)
        if blocks <= UNROLL:
            for s in range(blocks):
                sums = term(s, sums)
        else:
            sums = lax.fori_loop(0, blocks, term, sums)
        taps[rows, :], taps[irows, :] = sums
        return carry

    lax.fori_loop(0, block // SUB, chunk, 0)
    tap_grad = inverse(itab_ref, taps[...], block)[:medium] * (scale * factor)

    def finish(s):
        pair = jnp.concatenate([grad[2 * s], grad[2 * s + 1]], axis=1)
        time = inverse(itab_ref, pair, block) * scale
        for half in range(2):
            value = time[:, half * lanes : (half + 1) * lanes].astype(BF16).astype(F32)
            set_rows(tail, 2 * s + half, block, value)

    each(blocks // 2, finish)
    tail[total : total + 2 * SUB, :] = jnp.zeros((2 * SUB, lanes), F32)

    def span(b, sums):
        base = pl.multiple_of(b * height, height)
        values = saved_ref[b, 1].astype(F32)
        result = jnp.zeros((height, lanes), F32)
        new = []
        for j in range(short):
            shifted = tail[pl.ds(base + j, height), :]
            result = result + short_ref[j : j + 1, :].astype(F32) * shifted
            pieces = (values * shifted).reshape(height // SUB, SUB, lanes)
            new.append(sums[j] + jnp.sum(pieces, axis=0))
        out_ref[b] = result.astype(BF16)
        return tuple(new)

    start = tuple(jnp.zeros((SUB, lanes), F32) for _ in range(short))
    sums = lax.fori_loop(0, total // height, span, start)
    rows = [jnp.sum(value, axis=0, keepdims=True) * factor for value in sums]
    rest = taps_ref.shape[0] - medium
    rows.append(jnp.zeros((rest - short, lanes), F32))
    taps_ref[:medium, :] = tap_grad.astype(BF16)
    taps_ref[medium:, :] = jnp.concatenate(rows, axis=0).astype(BF16)


def call(kernel, outs, scratch, flops, *args):
    def whole(shape, place=None):
        place = place or (0,) * len(shape)
        return pl.BlockSpec(shape, lambda _: place, pipeline_mode=pl.Buffered(1))

    specs, values = [], []
    for arg in args:
        if isinstance(arg, tuple):
            arg, first, count = arg
            place = (0, first // count) + (0,) * (arg.ndim - 2)
            specs.append(whole(arg.shape[:1] + (count,) + arg.shape[2:], place))
        else:
            specs.append(whole(arg.shape))
        values.append(arg)
    return pl.pallas_call(
        kernel,
        out_shape=outs,
        grid=(1,),
        in_specs=specs,
        out_specs=jax.tree.map(lambda value: whole(value.shape), outs),
        scratch_shapes=scratch,
        compiler_params=pltpu.CompilerParams(vmem_limit_bytes=VMEM_LIMIT),
        cost_estimate=pl.CostEstimate(flops=flops, bytes_accessed=1 << 23, transcendentals=0),
    )(*values)


def pack_kernel(*refs):
    *ins, out_ref = refs
    outer, _, _, _, narrow = out_ref.shape
    for index, ref in enumerate(ins):
        for o in range(outer):
            out_ref[o, 0, index] = ref[:, o * narrow : (o + 1) * narrow]


def pack(values, outer, inner):
    height, channels = values[0].shape
    narrow = channels // (outer * inner)
    wide = channels // inner
    shape = (outer, inner, len(values), height, narrow)
    return pl.pallas_call(
        pack_kernel,
        out_shape=jax.ShapeDtypeStruct(shape, values[0].dtype),
        grid=(inner,),
        in_specs=[pl.BlockSpec((height, wide), lambda i: (0, i))] * len(values),
        out_specs=pl.BlockSpec((outer, 1) + shape[2:], lambda i: (0, i, 0, 0, 0)),
        cost_estimate=pl.CostEstimate(flops=1 << 28, bytes_accessed=1 << 22, transcendentals=0),
    )(*values)


def unpack(outer, inner, *groups):
    specs, values, outs, plan = [], [], [], []
    for value, order, wanted in groups:
        _, length, narrow = value.shape
        if order is None:
            values.append(value.reshape(outer, inner, length, narrow))
            specs.append(pl.BlockSpec((outer, 1, length, narrow), lambda i: (0, i, 0, 0)))
        else:
            values.append(value.reshape(inner, outer, length, narrow))
            specs.append(
                pl.BlockSpec((1, outer, length, narrow), lambda i, order=order: (order(i), 0, 0, 0))
            )
        for start, count, kind in wanted:
            outs.append(jax.ShapeDtypeStruct((count, outer * inner * narrow), kind))
            plan.append((len(values) - 1, order is None, start, count, narrow))

    def kernel(*refs):
        for (source, major, start, count, narrow), out_ref in zip(plan, refs[len(values) :]):
            for o in range(outer):
                place = (o, 0) if major else (0, o)
                part = refs[source][place + (slice(start, start + count),)]
                out_ref[:, o * narrow : (o + 1) * narrow] = part.astype(out_ref.dtype)

    return pl.pallas_call(
        kernel,
        out_shape=outs,
        grid=(inner,),
        in_specs=specs,
        out_specs=[pl.BlockSpec((o.shape[0], o.shape[1] // inner), lambda i: (0, i)) for o in outs],
        cost_estimate=pl.CostEstimate(flops=1 << 28, bytes_accessed=1 << 22, transcendentals=0),
    )(*values)


def gather(value, axis):
    count = lax.axis_size(axis)
    place = lax.axis_index(axis)
    result = jnp.stack([value] * count)
    for step in range(1, count):
        more = lax.ppermute(value, axis, [(s, (s + step) % count) for s in range(count)])
        result = lax.dynamic_update_index_in_dim(result, more, (place - step) % count, 0)
    return result


def trade(value, axis, dim):
    count = lax.axis_size(axis)
    place = lax.axis_index(axis)
    result = value
    for step in range(1, count):
        sent = lax.dynamic_index_in_dim(value, (place + step) % count, dim, keepdims=True)
        got = lax.ppermute(sent, axis, [(s, (s + step) % count) for s in range(count)])
        result = lax.dynamic_update_slice_in_dim(result, got, (place - step) % count, dim)
    return result


def swap(value, axes):
    return lax.all_to_all(value, axes, split_axis=0, concat_axis=0, tiled=True)


def per_device(
    out_grad,
    out_weight,
    outer_gate,
    long_out,
    inner_gate,
    conv_input,
    short_out,
    medium_out,
    long_filter,
    taps_short,
    taps_medium,
):
    height, channels = outer_gate.shape
    halves, lines, pairs, cores = (lax.axis_size(axis) for axis in ("h", "l", "j", "k"))
    groups = lax.axis_size("ch")
    outer = halves * lines
    inner = pairs * cores
    devices = outer * inner
    total = height * devices
    narrow = channels // devices
    wide = channels // inner
    medium, short = taps_medium.shape[0], taps_short.shape[0]
    planes = ("h", "l")
    seq = planes + ("j", "k")
    half, line = lax.axis_index("h"), lax.axis_index("l")
    me = half * lines + line
    my_inner = lax.axis_index("j") * cores + lax.axis_index("k")

    saved = pack([short_out, conv_input, inner_gate, medium_out, long_filter], outer, inner)
    saved = saved.reshape((devices,) + saved.shape[2:])

    both = gather(out_grad, "ch")
    both, saved = lax.optimization_barrier((both, saved))

    rows = out_weight.shape[0]
    depth = inner * groups * rows

    held = out_weight.reshape(rows, groups, inner, wide).transpose(2, 1, 0, 3)
    held = swap(held.reshape(inner * groups, rows, wide), ("j", "k", "ch"))
    held, saved = lax.optimization_barrier((held.reshape(depth, wide), saved))
    saved = swap(saved, seq)
    blocks = [(held, line)]
    for step in range(1, lines):
        more = lax.ppermute(held, "l", [(s, (s + step) % lines) for s in range(lines)])
        blocks.append((more, (line - step) % lines))

    share = height // groups
    first = lax.axis_index("ch") * share
    piece = lax.dynamic_slice(both, (1 - half, first, 0), (1, share, channels))
    piece = lax.ppermute(piece[0], "h", [(0, 1), (1, 0)])
    piece = gather(piece, "ch").reshape(height, channels)
    mine = lax.dynamic_index_in_dim(both, half, 0, keepdims=False)
    mine = gather(gather(mine, "j"), "k")
    mine = mine.reshape(inner * height, channels)
    other = gather(gather(piece, "j"), "k")
    other = other.reshape(inner * height, channels)

    def term(value, block, source):
        return dot(lax.dynamic_slice_in_dim(value, source * depth, depth, 1), block)

    away = sum(term(other, block, source) for block, source in blocks).astype(BF16)
    away = lax.ppermute(away, "h", [(0, 1), (1, 0)])
    hidden = sum(term(mine, block, source) for block, source in blocks) + away.astype(F32)
    hidden = hidden.reshape(cores, pairs, height, wide).transpose(1, 0, 2, 3)

    def to_plane(value):
        return value.reshape(height, pairs, cores, wide).transpose(1, 2, 0, 3)

    piece, outer_gate, long_out = lax.optimization_barrier((piece, outer_gate, long_out))
    gates = jnp.stack([to_plane(outer_gate), to_plane(long_out)], axis=2)
    gates = trade(trade(gates, "j", 0), "k", 1).astype(F32)
    long_grad = (hidden * gates[:, :, 0]).astype(BF16).reshape(inner * height, outer, narrow)
    long_grad, saved = lax.optimization_barrier((long_grad.transpose(1, 0, 2), saved))
    long_grad = swap(long_grad, planes).reshape(total, narrow)
    grad_outer = (hidden * gates[:, :, 1]).astype(BF16)
    grad_outer = trade(trade(grad_outer, "j", 0), "k", 1)
    grad_outer = grad_outer.transpose(2, 0, 1, 3).reshape(height, channels)

    first = (my_inner * outer + me) * narrow
    my_medium = lax.dynamic_slice_in_dim(taps_medium, first, narrow, 1)
    my_short = lax.dynamic_slice_in_dim(taps_short, first, narrow, 1)

    saved = jnp.pad(saved, [(0, 0)] * 3 + [(0, -narrow % LANES)])
    lanes = -(-narrow // LANES) * LANES

    def pad(value):
        return jnp.pad(value, [(0, 0)] * (value.ndim - 1) + [(0, lanes - narrow)])

    block = max(height, min(BLOCK, total // 2))
    blocks = total // block
    high, low = table(block)
    ftab = jnp.concatenate([high, low])
    itab = jnp.concatenate([high.T, low.T])
    factor = total ** (-0.5)
    spectra = pltpu.VMEM((blocks, 2 * block, lanes), F32)
    hold = pltpu.VMEM((blocks, 2 * SUB, lanes), F32)
    out = jax.ShapeDtypeStruct
    medium_grad, sent_long = call(
        functools.partial(long_kernel, factor / block),
        (out((total, lanes), BF16), out((devices, 2, height, lanes), BF16)),
        [spectra] * 3 + [hold],
        24 * 2 * block * total * lanes,
        (saved, 2, 2),
        (saved, 4, 1),
        pad(long_grad),
        ftab,
        itab,
    )
    rest = -(-short // 16) * 16
    sent_short, tap_grads = call(
        functools.partial(short_kernel, 1.0 / block, factor),
        (out((devices, height, lanes), BF16), out((medium + rest, lanes), BF16)),
        [spectra] * 2
        + [pltpu.VMEM((2 * block, lanes), F32), pltpu.VMEM((total + 2 * SUB, lanes), F32)],
        16 * 2 * block * total * lanes,
        medium_grad,
        (saved, 0, 2),
        pad(my_medium),
        pad(my_short),
        ftab,
        itab,
    )
    sent_long = sent_long.reshape(devices, 2 * height, lanes)
    got_long = swap(sent_long[..., :narrow], seq)
    tap_grads = tap_grads[:, :narrow]
    for axis in ("l", "h"):
        tap_grads = gather(tap_grads, axis)
    got_long, sent_short = lax.optimization_barrier((got_long, sent_short))
    grad_inner, grad_filter = unpack(
        outer, inner, (got_long, None, [(0, height, BF16), (height, height, F32)])
    )
    tap_grads, grad_inner = lax.optimization_barrier((tap_grads, grad_inner))
    for axis in ("j", "k"):
        tap_grads = gather(tap_grads, axis)
    got_short = swap(sent_short[..., :narrow], seq)
    grad_input, grad_medium, grad_short = unpack(
        outer,
        inner,
        (got_short, None, [(0, height, BF16)]),
        (
            tap_grads.reshape(devices, -1, narrow),
            lambda i: i % cores * pairs + i // cores,
            [(0, medium, F32), (medium, short, F32)],
        ),
    )
    return grad_outer, grad_inner, grad_input, grad_filter, grad_short, grad_medium


def solution(mesh):
    devices, groups = mesh.shape["seq"], mesh.shape["ch"]
    inner = 2 ** ((devices.bit_length() - 1) // 2)
    cores = min(2, inner)
    fine = Mesh(
        mesh.devices.reshape(2, devices // inner // 2, inner // cores, cores, groups),
        ("h", "l", "j", "k", "ch"),
    )
    seq = ("h", "l", "j", "k")
    tokens = P(seq, "ch")
    taps = P(None, "ch")

    step = jax.shard_map(
        per_device,
        mesh=fine,
        in_specs=(tokens, P(seq + ("ch",), None)) + (tokens,) * 7 + (taps, taps),
        out_specs=(tokens,) * 4 + (taps, taps),
        check_vma=False,
    )
    if max(fine.shape[axis] for axis in ("l", "j", "k")) > 2:
        return step
    return step
```
